512 devices in a mesh: rows: 32 (over x_lo, z), ka: 16 (over x_hi, y, core).
Axes of the slice: x: 4 (x_hi: 2, x_lo: 2; x = x_hi * 2 + x_lo), y: 4, z: 16, core: 2. Of those that a mesh axis runs over, the one named last changes fastest.
Arguments:
- pair_repr: bfloat16 [512, 512, 128], P('rows', 'ka'), may hold values from -6 to 6
- pair_mask: int32 [512, 512], P('rows', 'ka'), may hold values 0 or 1
- ln_gain: float32 [128], replicated, may hold values from 0.1 to 1.9
- ln_bias: float32 [128], replicated, may hold values from -3 to 3
- w_proj: bfloat16 [128, 256], replicated, may hold values from -0.5 to 0.5
- w_gate: bfloat16 [128, 256], replicated, may hold values from -0.5 to 0.5
- w_out_gate: bfloat16 [128, 128], replicated, may hold values from -0.5 to 0.5
- out_gain: float32 [128], replicated, may hold values from 0.1 to 1.9
- out_bias: float32 [128], replicated, may hold values from -3 to 3
- w_out: bfloat16 [128, 128], replicated, may hold values from -0.5 to 0.5
Outputs:
- update: bfloat16 [512, 512, 128], P('rows', 'ka')
The draws below stay inside these ranges and needn't reach their ends.
All inputs are finite; a program needn't handle non-finite values. No bound on the sum of `pair_mask` on one device may be relied on, other than what follows from the above.
Results may differ from the reference program's by a relative error of at most 0.015.
Values may be sent and summed in bfloat16 or wider, within the bound.
A program may use at most 64 MiB of HBM per device.

```python
import jax
import jax.numpy as jnp
from jax import lax

C = 128
H = 128
N = 512


def place_ends(drawn, own_key, smallest, high):
    spot = [jax.random.randint(jax.random.fold_in(own_key, axis), (), 0, length) for axis, length in enumerate(drawn.shape)]
    widest = drawn.shape.index(max(drawn.shape))
    beside = spot[:widest] + [(spot[widest] + 1) % drawn.shape[widest]] + spot[widest + 1:]
    return drawn.at[tuple(spot)].set(smallest).at[tuple(beside)].set(high)


def shard_levels(own_key, extent, shards, least, high):
    def one(position, parts):
        steps = jax.random.uniform(jax.random.fold_in(jax.random.fold_in(own_key, 6), position), (parts,), jnp.float32, least / len(shards), high / len(shards))
        return jnp.repeat(jnp.exp(steps), extent[position] // parts).reshape((-1,) + (1,) * (len(extent) - position - 1))

    loudness = one(*shards[0])
    for cut in shards[1:]:
        loudness = loudness * one(*cut)
    return loudness


def bell_draw(key, dims, deviation, reach, shards=(), held_as=jnp.bfloat16):
    array = jax.random.normal(key, dims, jnp.float32) * deviation
    if len(shards) > 0:
        array = shard_levels(key, dims, shards, -0.22, 0.18) * array
    return jnp.clip(array, min=-reach, max=reach).astype(held_as)


def setup_inputs(seed: int = 0) -> dict:
    seeds = jax.random.split(jax.random.key(seed), 11)
    pair_repr = bell_draw(seeds[0], (N, N, C), 1.0, 6.0, ((0, 32), (1, 16)))
    pair_mask = place_ends((jax.random.randint(seeds[1], (N, N), 0, 4) < 3).astype(jnp.int32), jax.random.fold_in(seeds[1], 1), 0, 1)
    ln_gain = jnp.clip(1.0 + 0.18 * jax.random.normal(seeds[2], (C,), jnp.float32), 0.1, 1.9)
    ln_bias = bell_draw(seeds[3], (C,), 0.5, 3.0, (), jnp.float32)
    w_proj = bell_draw(seeds[4], (C, 2 * H), C ** -0.5, 0.5)
    w_gate = bell_draw(seeds[5], (C, 2 * H), C ** -0.5, 0.5)
    w_out_gate = bell_draw(seeds[6], (C, C), C ** -0.5, 0.5)
    out_gain = jnp.clip(1.0 + 0.18 * jax.random.normal(seeds[7], (H,), jnp.float32), 0.1, 1.9)
    out_bias = bell_draw(seeds[8], (H,), 0.5, 3.0, (), jnp.float32)
    w_out = bell_draw(seeds[9], (H, C), H ** -0.5, 0.5)
    return dict(pair_repr=pair_repr, pair_mask=pair_mask, ln_gain=ln_gain, ln_bias=ln_bias, w_proj=w_proj, w_gate=w_gate, w_out_gate=w_out_gate, out_gain=out_gain, out_bias=out_bias, w_out=w_out)


def layer_norm(values, gain_vec, bias_vec):
    center = lax.optimization_barrier(jnp.mean(values, axis=-1, keepdims=True))
    deviate = values - center
    spread = lax.optimization_barrier(jnp.mean(deviate * deviate, axis=-1, keepdims=True))
    return deviate * lax.rsqrt(spread + 1e-05) * gain_vec + bias_vec

def reference(pair_repr, pair_mask, ln_gain, ln_bias, w_proj, w_gate, w_out_gate, out_gain, out_bias, w_out):
    normed = layer_norm(pair_repr.astype(jnp.float32), ln_gain, ln_bias).astype(jnp.bfloat16)
    flat_rows = normed.reshape(N * N, C)
    projected = jnp.dot(flat_rows, w_proj, preferred_element_type=jnp.float32)
    gate_logits = jnp.dot(flat_rows, w_gate, preferred_element_type=jnp.float32)
    mask_col = pair_mask.reshape(N * N, 1).astype(jnp.float32)
    edges = (jax.nn.sigmoid(gate_logits) * projected * mask_col).astype(jnp.bfloat16).reshape(N, N, 2 * H)
    left_edge = jnp.transpose(edges[:, :, :H], (2, 0, 1)).astype(jnp.float32)
    right_edge = jnp.transpose(edges[:, :, H:], (2, 1, 0)).astype(jnp.float32)
    triangle = jnp.transpose(jnp.matmul(left_edge, right_edge), (1, 2, 0))
    tri_normed = layer_norm(triangle, out_gain, out_bias).astype(jnp.bfloat16)
    out_gate = jax.nn.sigmoid(jnp.dot(flat_rows, w_out_gate, preferred_element_type=jnp.float32))
    projected_out = jnp.dot(tri_normed.reshape(N * N, H), w_out, preferred_element_type=jnp.float32)
    return (out_gate * projected_out).astype(jnp.bfloat16).reshape(N, N, C)
```

```python
import jax
import jax.numpy as jnp
from jax import lax
from jax.experimental import pallas as pl
from jax.experimental.pallas import tpu as pltpu
from jax.sharding import PartitionSpec as P

MESH = pl.DeviceIdType.MESH
F32 = jnp.float32
BF16 = jnp.bfloat16
NT = (((1,), (1,)), ((), ()))
ZN = 16
PLANE = 32
KAN = 16
EPS = 1e-05


def iota(shape, dim):
    return lax.broadcasted_iota(jnp.int32, shape, dim)


def dot_nt(a, b):
    return lax.dot_general(a, b, NT, preferred_element_type=F32)


def chunk_swap(tiles, chunk):
    for bit, width in ((1, 32), (2, 64)):
        low = (chunk & bit) == 0
        swapped = []
        for e in range(4):
            other = tiles[e ^ bit]
            if e & bit:
                swapped.append(jnp.where(low, pltpu.roll(other, 128 - width, 1), tiles[e]))
            else:
                swapped.append(jnp.where(low, tiles[e], pltpu.roll(other, width, 1)))
        tiles = swapped
    return tiles


def kernel(
    pair, mask, gain, bias, w_proj, w_gate, w_out_gate, out_gain, out_bias, w_out, out,
    normed, stage, send_r, send_l, recv_l, ring, left_m, right_m, packed, send_o, recv_o,
    gate_s, gain_t, bias_t, flat,
    sem_r, sem_rs, sem_l, sem_ls, sem_ring, sem_up, sem_dn, sem_o, sem_os,
):
    rows = lax.axis_index("rows")
    ka = lax.axis_index("ka")
    xlo = rows // ZN
    z = rows % ZN
    me = xlo * KAN + ka
    mine_c = ka // 4
    mine_s = xlo * 4 + ka % 4
    up = {"rows": xlo * ZN + (z + 1) % ZN, "ka": ka}
    down = {"rows": xlo * ZN + (z + ZN - 1) % ZN, "ka": ka}

    def peer(t):
        d = (me + t) % PLANE
        return d, {"rows": (d // KAN) * ZN + z, "ka": d % KAN}

    barrier = pltpu.get_barrier_semaphore()

    @pl.loop(1, PLANE)
    def _(t):
        pl.semaphore_signal(barrier, inc=1, device_id=peer(t)[1], device_id_type=MESH)

    pl.semaphore_signal(barrier, inc=1, device_id=up, device_id_type=MESH)
    pl.semaphore_signal(barrier, inc=1, device_id=down, device_id_type=MESH)

    spread = (iota((32, 128), 1) % 32 == iota((32, 128), 0)).astype(BF16)
    wide = jnp.dot(mask[...].astype(F32).astype(BF16), spread, preferred_element_type=F32)
    wide = jnp.where(iota((16, 128), 1) // 32 == iota((16, 128), 0) % 4, wide, 0.0)
    group = (iota((8, 16), 1) // 4 == iota((8, 16), 0)).astype(BF16)
    mask_rows = jnp.dot(group, wide.astype(BF16), preferred_element_type=F32)

    for a in range(4):
        x = pair[4 * a : 4 * a + 4].reshape(128, 128).astype(F32)
        d = x - jnp.mean(x, axis=1, keepdims=True)
        v = jnp.mean(d * d, axis=1, keepdims=True)
        normed[128 * a : 128 * a + 128, :] = (d * lax.rsqrt(v + EPS) * gain[...] + bias[...]).astype(BF16)

    def edges(lo, send):
        wp = w_proj[:, lo : lo + 128].astype(F32).T.astype(BF16)
        wg = w_gate[:, lo : lo + 128].astype(F32).T.astype(BF16)
        for a in range(4):
            n = normed[128 * a : 128 * a + 128, :]
            e = jax.nn.sigmoid(dot_nt(wg, n)) * dot_nt(wp, n) * mask_rows[a : a + 1, :]
            stage[pl.ds(a, 128, stride=4), :] = e
        send[...] = stage[...].reshape(PLANE, 16, 128).astype(BF16)

    def exchange(send, landing, send_sem, recv_sem):
        @pl.loop(1, PLANE)
        def _(t):
            d, device = peer(t)
            pltpu.make_async_remote_copy(
                src_ref=send.at[d], dst_ref=landing, send_sem=send_sem, recv_sem=recv_sem,
                device_id=device, device_id_type=MESH,
            ).start()

        pltpu.make_async_copy(send.at[me], landing, recv_sem).start()

    edges(128, send_r)
    pl.semaphore_wait(barrier, PLANE + 1)
    exchange(send_r, ring.at[z, mine_c, mine_s], sem_rs, sem_r.at[mine_c])
    edges(0, send_l)
    exchange(send_l, recv_l.at[mine_c, mine_s], sem_ls, sem_l)

    def hop(block, c, sem, device):
        return pltpu.make_async_remote_copy(
            src_ref=ring.at[block, c], dst_ref=ring.at[block, c], send_sem=sem,
            recv_sem=sem_ring.at[block, c], device_id=device, device_id_type=MESH,
        )

    for c in range(4):
        pltpu.make_async_copy(ring.at[z, c], ring.at[z, c], sem_r.at[c]).wait()
        hop(z, c, sem_up, up).start()
        hop(z, c, sem_dn, down).start()

    chunk = iota((16, 128), 1) // 32

    def relay(tiles, place):
        tiles = tiles.astype(F32)
        for x in range(2):
            for b, t in enumerate(chunk_swap([tiles[4 * x + e] for e in range(4)], chunk)):
                place(x, b, t.astype(BF16))

    def relay_right(side, block, c):
        def place(x, b, t):
            row = 16 * (4 * x + b)
            right_m[side, row : row + 16, 128 * c : 128 * c + 128] = t

        relay(ring[block, c], place)

    row8 = iota((8, 128), 0)
    slot = (iota((8, 128), 1) // 4) % 4
    lane_low = iota((32, 128), 1) < 64

    def products(side, block):
        prod = dot_nt(left_m[...], right_m[side])
        for v in range(4):
            total = jnp.zeros((8, 128), F32)
            for b in range(4):
                piece = prod[32 * b + 8 * v : 32 * b + 8 * v + 8]
                for half in range(2):
                    h = 2 * (v % 2) + half
                    moved = piece if b == h else pltpu.roll(piece, (4 * (b - h)) % 128, 1)
                    total = jnp.where((row8 // 4 == half) & (slot == b), moved, total)
            packed[block, 8 * v : 8 * v + 8, :] = total

    def send_pair(t):
        odd = (z + t) % 2
        q = ((odd * (z + t) + (1 - odd) * (z - t + ZN)) % ZN) // 2
        even_p = packed[2 * q]
        odd_p = packed[2 * q + 1]
        sends = (
            jnp.where(lane_low, even_p, pltpu.roll(odd_p, 64, 1)),
            jnp.where(lane_low, pltpu.roll(even_p, 64, 1), odd_p),
        )
        for xj in range(2):
            for xi in range(2):
                at = 4 * q + 2 * xj + xi
                send_o[at] = sends[xj][16 * xi : 16 * xi + 16].astype(BF16)
        for xj in range(2):
            for xi in range(2):
                at = 4 * q + 2 * xj + xi
                target = xi * KAN + xj * 8 + q

                @pl.when(target != me)
                def _():
                    pltpu.make_async_remote_copy(
                        src_ref=send_o.at[at], dst_ref=recv_o.at[me], send_sem=sem_os, recv_sem=sem_o,
                        device_id={"rows": xi * ZN + z, "ka": xj * 8 + q}, device_id_type=MESH,
                    ).start()

                @pl.when(target == me)
                def _():
                    pltpu.make_async_copy(send_o.at[at], recv_o.at[me], sem_o).start()

    for c in range(4):
        relay_right(0, z, c)
    pltpu.make_async_copy(recv_l, recv_l, sem_l).wait()
    for c in range(4):
        def place(x, b, t):
            row = 16 * (2 * b + x)
            left_m[row : row + 16, 128 * c : 128 * c + 128] = t

        relay(recv_l[c], place)
    products(0, z)

    gain_t[...] = jnp.broadcast_to(out_gain[...], (128, 128)).T
    bias_t[...] = jnp.broadcast_to(out_bias[...], (128, 128)).T
    gate_s[...] = jax.nn.sigmoid(jnp.dot(normed[...], w_out_gate[...], preferred_element_type=F32))

    @pl.loop(1, 8)
    def _(t):
        zu = (z - t + ZN) % ZN
        zd = (z + t) % ZN
        for c in range(4):
            hop(zu, c, sem_up, up).wait_recv()
            if c < 2:
                hop(zu, c, sem_up, up).start()
            else:
                @pl.when(t < 7)
                def _():
                    hop(zu, c, sem_up, up).start()
            hop(zd, c, sem_dn, down).wait_recv()
            if c >= 2:
                hop(zd, c, sem_dn, down).start()
            else:
                @pl.when(t < 7)
                def _():
                    hop(zd, c, sem_dn, down).start()
            relay_right(0, zu, c)
            relay_right(1, zd, c)
        products(0, zu)
        products(1, zd)
        send_pair(t)

    far = (z + 8) % ZN
    for c in range(4):
        hop(far, c, sem_up, up).wait_recv()
        relay_right(0, far, c)
    products(0, far)
    send_pair(8)

    r = iota((128, 128), 0)
    source = ((r // 16) % 2) * 64 + (r % 4) * 16 + (r // 32) * 4 + (r // 4) % 4
    turn = (iota((128, 128), 1) == source).astype(F32).astype(BF16)

    pltpu.make_async_copy(recv_o, recv_o, sem_o).wait()
    flat[...] = recv_o[...].reshape(512, 128).astype(F32)
    for a in range(4):
        y = flat[pl.ds(a, 128, stride=4), :]
        d = y - jnp.mean(y, axis=0, keepdims=True)
        v = jnp.mean(d * d, axis=0, keepdims=True)
        n = (d * lax.rsqrt(v + EPS) * gain_t[...] + bias_t[...]).astype(BF16)
        turned = dot_nt(turn, n).astype(BF16)
        proj = jnp.dot(turned, w_out[...], preferred_element_type=F32)
        result = (gate_s[128 * a : 128 * a + 128, :] * proj).astype(BF16)
        out[4 * a : 4 * a + 4] = result.reshape(4, 32, 128)

    pltpu.make_async_copy(send_r.at[pl.ds(0, 31)], send_r.at[pl.ds(0, 31)], sem_rs).wait()
    pltpu.make_async_copy(send_l.at[pl.ds(0, 31)], send_l.at[pl.ds(0, 31)], sem_ls).wait()
    pltpu.make_async_copy(send_o.at[pl.ds(0, 31)], send_o.at[pl.ds(0, 31)], sem_os).wait()
    sent = ring.at[pl.ds(0, 15), pl.ds(0, 2)]
    pltpu.make_async_copy(sent, sent, sem_up).wait()
    pltpu.make_async_copy(sent, sent, sem_dn).wait()


def body(
    pair_repr, pair_mask, ln_gain, ln_bias, w_proj, w_gate, w_out_gate, out_gain, out_bias, w_out
):
    dma = pltpu.SemaphoreType.DMA
    vmem = pl.BlockSpec(memory_space=pltpu.VMEM)
    row = lambda v: v.reshape(1, 128)
    return pl.pallas_call(
        kernel,
        out_shape=jax.ShapeDtypeStruct((16, 32, 128), BF16),
        in_specs=[vmem] * 10,
        out_specs=vmem,
        scratch_shapes=[
            pltpu.VMEM((512, 128), BF16),
            pltpu.VMEM((512, 128), F32),
            pltpu.VMEM((PLANE, 16, 128), BF16),
            pltpu.VMEM((PLANE, 16, 128), BF16),
            pltpu.VMEM((4, 8, 16, 128), BF16),
            pltpu.VMEM((ZN, 4, 8, 16, 128), BF16),
            pltpu.VMEM((128, 512), BF16),
            pltpu.VMEM((2, 128, 512), BF16),
            pltpu.VMEM((ZN, 32, 128), F32),
            pltpu.VMEM((PLANE, 16, 128), BF16),
            pltpu.VMEM((PLANE, 16, 128), BF16),
            pltpu.VMEM((512, 128), F32),
            pltpu.VMEM((128, 128), F32),
            pltpu.VMEM((128, 128), F32),
            pltpu.VMEM((512, 128), F32),
            dma((4,)),
            dma,
            dma,
            dma,
            dma((ZN, 4)),
            dma,
            dma,
            dma,
            dma,
        ],
        compiler_params=pltpu.CompilerParams(collective_id=0, has_side_effects=True),
        name="triangle",
    )(
        pair_repr, pair_mask, row(ln_gain), row(ln_bias), w_proj, w_gate, w_out_gate,
        row(out_gain), row(out_bias), w_out,
    )


def solution(mesh):
    spread = P("rows", "ka", None)
    placed = (spread, P("rows", "ka")) + (P(),) * 8
    return jax.shard_map(body, mesh=mesh, in_specs=placed, out_specs=spread, check_vma=False)
```
